32 devices in a mesh: sfc: 8 (over z, core), lev: 4 (over y, x).
Axes of the slice: x: 2, y: 2, z: 4, core: 2. Of those that a mesh axis runs over, the one named last changes fastest.
Arguments:
- tracer_old: float32 [4, 10, 16, 3072], P('lev', None, None, 'sfc'), may hold values from 0.1 to 2
- air_old: float32 [4, 16, 3072], P('lev', None, 'sfc'), may hold values from 0.3 to 20, as said below
- air_new: float32 [4, 16, 3072], P('lev', None, 'sfc'), may hold values from 0.4 to 20, as said below
- dep_coord: float32 [2, 4, 16, 3072], P(None, 'lev', None, 'sfc'), may hold values from -1 to 1
- dep_slot: int32 [4, 16, 3072], P('lev', None, 'sfc'), may hold values from 0 to 639
- fetch_list: int32 [8, 2, 128], P('sfc'), may hold values from 0 to 383, as said below
Outputs:
- tracer_new: float32 [4, 10, 16, 3072], P('lev', None, None, 'sfc')
The draws below stay inside these ranges and needn't reach their ends.
Inputs may be any that keep to these rules, and one draw needn't show every extreme that they name: `fetch_list`: side 0 holds distinct indices in [128, 384); side 1 holds distinct indices in [0, 256). `air_old`: positive. `air_new`: positive.
All inputs are finite; a program needn't handle non-finite values.
Results may differ from the reference program's by a relative error of at most 0.0003.
Values sent between devices are 32-bit elements; how exact they have to be, the bound alone decides.
A program may use at most 64 MiB of HBM per device.

```python
import math
import jax
import jax.numpy as jnp
from jax import lax

NP2 = 16
TRACERS = 10
E_DEV = 384
CAP = 128
BAND = 256
SEGS = 8
ELEMS = 3072
LEVELS = 4


def air_ramp():
    levels = jnp.arange(LEVELS, dtype=jnp.float32)
    elems = jnp.arange(ELEMS, dtype=jnp.float32)
    down = 1.0 + 2.0 * levels / max(LEVELS - 1, 1)
    along = 1.0 + 2.0 * elems / ELEMS
    return down[:, None, None] * along[None, None, :]


def draw_air_old(key, part):
    shape = (LEVELS, NP2, ELEMS)
    common = jax.random.uniform(jax.random.fold_in(key, 5), (), jnp.float32, 0.75, 1.25)
    base = jax.random.uniform(key, shape, jnp.float32, 0.8, 1.2)
    return common * base * air_ramp()


def draw_air_new(key, part):
    shape = (LEVELS, NP2, ELEMS)
    inner = jax.random.fold_in(key, 7)
    base = jax.random.uniform(inner, shape, jnp.float32, 0.72, 1.08)
    return base * air_ramp()


def draw_fetch_list(key, part):
    keys = jax.random.split(jax.random.fold_in(key, 11), SEGS * 2)
    orders = jax.vmap(lambda k: jax.random.permutation(k, BAND))(keys)
    picked = orders[:, :CAP].reshape(SEGS, 2, CAP).astype(jnp.int32)
    offset = jnp.array([E_DEV - BAND, 0], dtype=jnp.int32)
    return picked + offset[None, :, None]


def with_ends(values, key, smallest, high):
    longest = values.shape.index(max(values.shape))
    spots = []
    for shift in (0, 1):
        where = [jax.random.randint(jax.random.fold_in(key, axis), (), 0, length) for axis, length in enumerate(values.shape)]
        where[longest] = (where[longest] + shift) % values.shape[longest]
        spots.append(tuple(where))
    return values.at[spots[0]].set(smallest).at[spots[1]].set(high)


def level_of(own_key, dims, shards, smallest, largest):
    factor_of, own = 1.0, jax.random.fold_in(own_key, 6)
    for axis_at, blocks in shards:
        draws = jnp.exp(jax.random.uniform(jax.random.fold_in(own, axis_at), (blocks,), jnp.float32, smallest / len(shards), largest / len(shards)))
        factor_of = factor_of * jnp.repeat(draws, dims[axis_at] // blocks).reshape([-1 if axis == axis_at else 1 for axis in range(len(dims))])
    return factor_of


def setup_inputs(seed: int = 0) -> dict:
    splits = jax.random.split(jax.random.key(seed), 7)
    tracer_old = jnp.clip(jnp.exp(math.log(2.0) - 2.9957323 * jax.random.uniform(splits[0], (LEVELS, TRACERS, NP2, ELEMS), jnp.float32) ** level_of(splits[0], (LEVELS, TRACERS, NP2, ELEMS), ((0, 4), (3, 8)), -0.2, 0.2)), 0.1, 2.0)
    air_old = draw_air_old(jax.random.fold_in(splits[6], 71), 0)
    air_new = draw_air_new(jax.random.fold_in(splits[6], 71), 0)
    dep_coord = jnp.clip(jax.random.uniform(splits[3], (2, LEVELS, NP2, ELEMS), jnp.float32, -1.0, 1.0) * level_of(splits[3], (2, LEVELS, NP2, ELEMS), ((1, 4), (3, 8)), -0.4, 0.0), -1.0, 1.0)
    dep_slot = with_ends(jax.random.randint(splits[4], (LEVELS, NP2, ELEMS), 0, E_DEV + 2 * CAP), jax.random.fold_in(splits[4], 1), 0, (E_DEV + 2 * CAP) - 1).astype(jnp.int32)
    fetch_list = draw_fetch_list(jax.random.fold_in(splits[6], 71), 0)
    return dict(tracer_old=tracer_old, air_old=air_old, air_new=air_new, dep_coord=dep_coord, dep_slot=dep_slot, fetch_list=fetch_list)


NODES = (-1.0, -0.4472135954999579, 0.4472135954999579, 1.0)


def basis(coord):
    terms = []
    for first in range(4):
        term = jnp.ones_like(coord)
        for other in range(4):
            if other != first:
                term = term * (coord - NODES[other]) / (NODES[first] - NODES[other])
        terms.append(term)
    return jnp.stack(terms)


def weights(coord_a, coord_b):
    along_a = basis(coord_a)
    along_b = basis(coord_b)
    stacked = along_a[:, None] * along_b[None, :]
    return stacked.reshape((16,) + coord_a.shape)


def reference(tracer_old, air_old, air_new, dep_coord, dep_slot, fetch_list):
    segs = fetch_list.shape[0]
    total = tracer_old.shape[3]
    e_dev = total // segs
    seg_ids = jnp.arange(segs, dtype=jnp.int32)
    own = seg_ids[:, None] * e_dev + jnp.arange(e_dev, dtype=jnp.int32)[None, :]
    left = ((seg_ids - 1) % segs)[:, None] * e_dev + fetch_list[:, 0]
    right = ((seg_ids + 1) % segs)[:, None] * e_dev + fetch_list[:, 1]
    table = jnp.concatenate([own, left, right], axis=1).astype(jnp.int32)
    seg_of = (jnp.arange(total, dtype=jnp.int32) // e_dev).astype(jnp.int32)
    source = table[seg_of[None, None, :], dep_slot]

    def level(items):
        field, src, coord_a, coord_b = items

        def point(inner):
            index, along_a, along_b = inner
            blocks = jnp.take(field, index, axis=2)
            wts = weights(along_a, along_b)
            value = jnp.sum(wts[None] * blocks, axis=1)
            return value, jnp.min(blocks, axis=1), jnp.max(blocks, axis=1)

        return lax.map(point, (src, coord_a, coord_b))

    interp, low, high = lax.map(level, (tracer_old, source, dep_coord[0], dep_coord[1]))
    interp = jnp.moveaxis(interp, 1, 2)
    low = jnp.moveaxis(low, 1, 2)
    high = jnp.moveaxis(high, 1, 2)
    clipped = jnp.clip(interp, low, high)
    mass_new = air_new[:, None]
    old_mass = jnp.sum(air_old[:, None] * tracer_old, axis=(0, 2, 3))
    clip_mass = jnp.sum(mass_new * clipped, axis=(0, 2, 3))
    room_up = jnp.sum(mass_new * (high - clipped), axis=(0, 2, 3))
    room_down = jnp.sum(mass_new * (clipped - low), axis=(0, 2, 3))
    shortfall = (old_mass - clip_mass)[None, :, None, None]
    raised = shortfall * (high - clipped) / room_up[None, :, None, None]
    lowered = shortfall * (clipped - low) / room_down[None, :, None, None]
    return clipped + jnp.where(shortfall >= 0, raised, lowered)
```

```python
import functools

import jax
import jax.numpy as jnp
from jax import lax
from jax.experimental import pallas as pl
from jax.experimental.pallas import tpu as pltpu
from jax.sharding import PartitionSpec as P

BAND = 256
LANES = 128
SUB = 8
NODES = (-1.0, -0.4472135954999579, 0.4472135954999579, 1.0)
MESH = pl.DeviceIdType.MESH


def basis(coord):
    terms = []
    for first in range(4):
        term = None
        scale = 1.0
        for other in range(4):
            if other != first:
                factor = coord - NODES[other]
                term = factor if term is None else term * factor
                scale = scale / (NODES[first] - NODES[other])
        terms.append(term * scale)
    return terms


def lookup(values, index):
    return jnp.take_along_axis(values, index, axis=1, mode="promise_in_bounds")


def wide(row):
    return jnp.broadcast_to(row, (SUB, LANES))


def kernel(
    sizes, tr, air_old, air_new, coord, slot, fetch, out,
    natural, table, halo, side, part, along_a, along_b, places, masses, kept, message, heard,
    halo_send, halo_recv, sum_send, sum_recv,
):
    n_sfc, n_lev = sizes
    n_all = n_sfc * n_lev
    points = slot.shape[0]
    e_dev = tr.shape[1]
    tracers = tr.shape[0] // points
    groups = e_dev // LANES
    row_groups = tr.shape[0] // SUB
    mains = points
    rests = row_groups - mains
    band_groups = BAND // LANES
    me_s, me_l = lax.axis_index("sfc"), lax.axis_index("lev")
    me = me_s * n_lev + me_l

    def spot(distance):
        other = lax.rem(me + distance, n_all)
        return (lax.div(other, n_lev), lax.rem(other, n_lev))

    barrier = pltpu.get_barrier_semaphore()

    def greet(distance, carry):
        pl.semaphore_signal(barrier, inc=1, device_id=spot(distance), device_id_type=MESH)
        return carry

    lax.fori_loop(1, n_all, greet, 0)

    def cols(group):
        return pl.ds(group * LANES, LANES)

    def picked_rows(group):
        if group < mains:
            return pl.ds(group, SUB, stride=points)
        return pl.ds(SUB * points + group - mains, SUB, stride=rests)

    for g in range(groups):
        natural[g] = tr[:, cols(g)]
    for r in range(row_groups):
        for g in range(groups):
            table[g, pl.ds(r * SUB, SUB), :] = natural[g, picked_rows(r), :]
    for i, term in enumerate(basis(coord[0])):
        for g in range(groups):
            term_g = term[:, g * LANES : (g + 1) * LANES]
            along_a[g, pl.ds(i, points, stride=SUB), :] = term_g
            along_a[g, pl.ds(i + 4, points, stride=SUB), :] = term_g
    for i, term in enumerate(basis(coord[1])):
        for g in range(groups):
            along_b[i, g] = term[:, g * LANES : (g + 1) * LANES]
    for g in range(groups):
        places[g] = slot[:, cols(g)]
        masses[g] = air_new[:, cols(g)]

    def own(n, carry):
        rows = [wide(places[g, pl.ds(n, 1), :]) for g in range(groups)]
        lows = [row & (LANES - 1) for row in rows]
        highs = [row >> 7 for row in rows]
        for r in range(row_groups):
            blocks = [table[g, pl.ds(r * SUB, SUB), :] for g in range(groups)]
            for e in range(groups):
                value = lookup(blocks[0], lows[e])
                for g in range(1, groups):
                    value = jnp.where(highs[e] == g, lookup(blocks[g], lows[e]), value)
                part[n, pl.ds(r * SUB, SUB), cols(e)] = value
        return carry

    pl.semaphore_wait(barrier, n_all - 1)
    right = (lax.rem(me_s + 1, n_sfc), me_l)
    left = (lax.rem(me_s + n_sfc - 1, n_sfc), me_l)
    sends = []
    for k, (target, start) in enumerate(((right, e_dev - BAND), (left, 0))):
        for g in range(band_groups):
            send = pltpu.make_async_remote_copy(
                src_ref=tr.at[:, pl.ds(start + g * LANES, LANES)],
                dst_ref=halo.at[k, g],
                send_sem=halo_send.at[k, g],
                recv_sem=halo_recv.at[k, g],
                device_id=target,
                device_id_type=MESH,
            )
            send.start()
            sends.append(send)

    lax.fori_loop(0, points, own, 0)
    old_main = jnp.zeros((SUB, LANES), jnp.float32)
    for j in range(mains):
        for g in range(groups):
            old_main += table[g, pl.ds(j * SUB, SUB), :] * wide(air_old[pl.ds(j, 1), cols(g)])
    old_rest = []
    for t in range(SUB, tracers):
        product = tr[pl.ds(t * points, points), :] * air_old[...]
        old_rest.append(jnp.sum(jnp.sum(product, axis=1, keepdims=True), axis=0, keepdims=True))

    for k in range(2):
        for g in range(band_groups):
            sends[k * band_groups + g].wait()
        index = wide(fetch[pl.ds(k, 1), :])
        if k == 0:
            index = index - (e_dev - BAND)
        index_low, index_high = index & (LANES - 1), index >> 7
        for r in range(row_groups):
            value = lookup(halo[k, 0, picked_rows(r), :], index_low)
            for g in range(1, band_groups):
                value = jnp.where(
                    index_high == g, lookup(halo[k, g, picked_rows(r), :], index_low), value
                )
            side[k, pl.ds(r * SUB, SUB), :] = value

    def finish(n, carry):
        sums = list(carry)
        for e in range(groups):
            row = wide(places[e, pl.ds(n, 1), :])
            low_index, high_index = row & (LANES - 1), row >> 7
            in_left, in_right = high_index == groups, high_index == groups + 1
            mass = wide(masses[e, pl.ds(n, 1), :])

            def point(r):
                here = pl.ds(r * SUB, SUB)
                value = part[n, here, cols(e)]
                value = jnp.where(in_left, lookup(side[0, here, :], low_index), value)
                return jnp.where(in_right, lookup(side[1, here, :], low_index), value)

            terms_b = [wide(along_b[m, e, pl.ds(n, 1), :]) for m in range(4)]
            interp = low = high = None
            for i in range(4):
                inner = None
                for m in range(4):
                    value = point(4 * i + m)
                    low = value if low is None else jnp.minimum(low, value)
                    high = value if high is None else jnp.maximum(high, value)
                    scaled = terms_b[m] * value
                    inner = scaled if inner is None else inner + scaled
                term_a = wide(along_a[e, pl.ds(n * SUB + i, 1), :])
                inner = inner * term_a
                interp = inner if interp is None else interp + inner
            rest = low_rest = high_rest = None
            for q in range(rests):
                value = point(mains + q)
                low_rest = value if low_rest is None else jnp.minimum(low_rest, value)
                high_rest = value if high_rest is None else jnp.maximum(high_rest, value)
                scaled = terms_b[q] * value
                rest = scaled if rest is None else rest + scaled
            rest = rest * along_a[e, pl.ds(n * SUB, SUB), :]
            for shift in (1, 2):
                rest = rest + pltpu.roll(rest, SUB - shift, 0)
                low_rest = jnp.minimum(low_rest, pltpu.roll(low_rest, SUB - shift, 0))
                high_rest = jnp.maximum(high_rest, pltpu.roll(high_rest, SUB - shift, 0))
            for b, (value, least, most) in enumerate(
                ((interp, low, high), (rest, low_rest, high_rest))
            ):
                clipped = jnp.minimum(jnp.maximum(value, least), most)
                up, down = most - clipped, clipped - least
                for q, kind in enumerate((clipped, up, down)):
                    kept[b, q, n, :, cols(e)] = kind
                    sums[3 * b + q] = sums[3 * b + q] + mass * kind
        return tuple(sums)

    zero = jnp.zeros((SUB, LANES), jnp.float32)
    sums = lax.fori_loop(0, points, finish, (zero,) * 6)

    lane = lax.broadcasted_iota(jnp.int32, (SUB, LANES), 1)
    row = lax.broadcasted_iota(jnp.int32, (SUB, LANES), 0)
    packed = jnp.where(lane == 0, jnp.sum(old_main, axis=1, keepdims=True), 0.0)
    for b in range(2):
        for q in range(3):
            total = jnp.sum(sums[3 * b + q], axis=1, keepdims=True)
            packed = jnp.where(lane == 4 * b + q + 1, total, packed)
    for k, total in enumerate(old_rest):
        packed = jnp.where((lane == 4) & (row == 4 * k), total, packed)
    message[...] = packed

    def tell(distance, carry):
        pltpu.make_async_remote_copy(
            src_ref=message,
            dst_ref=heard.at[distance - 1],
            send_sem=sum_send,
            recv_sem=sum_recv,
            device_id=spot(distance),
            device_id_type=MESH,
        ).start()
        return carry

    lax.fori_loop(1, n_all, tell, 0)
    pltpu.make_async_copy(heard, heard, sum_recv).wait()
    total = packed
    for k in range(n_all - 1) if n_all <= 64 else ():
        total = total + heard[k]
    if n_all > 64:
        total = lax.fori_loop(0, n_all - 1, lambda k, acc: acc + heard[k], total)

    ups, gains = [], []
    for b in range(2):
        old, clip, up, down = [total[:, 4 * b + q : 4 * b + q + 1] for q in range(4)]
        shortfall = jnp.broadcast_to(old - clip, (SUB, LANES))
        is_up = shortfall >= 0
        room = jnp.where(is_up, jnp.broadcast_to(up, (SUB, LANES)), jnp.broadcast_to(down, (SUB, LANES)))
        ups.append(is_up)
        gains.append(shortfall / room)

    def fix(n, carry):
        for e in range(groups):
            done = []
            for b in range(2):
                clipped, up, down = [kept[b, q, n, :, cols(e)] for q in range(3)]
                done.append(clipped + gains[b] * jnp.where(ups[b], up, down))
            natural[e, pl.ds(n, SUB, stride=points), :] = done[0]
            for t in range(SUB, tracers):
                at = 4 * (t - SUB)
                natural[e, pl.ds(t * points + n, 1), :] = done[1][at : at + 1]
        return carry

    lax.fori_loop(0, points, fix, 0)
    for g in range(groups):
        out[:, cols(g)] = natural[g]
    pltpu.make_async_copy(heard, heard, sum_send).wait()


def solution(mesh):
    sizes = (mesh.shape["sfc"], mesh.shape["lev"])
    n_all = sizes[0] * sizes[1]

    def on_device(tracer_old, air_old, air_new, dep_coord, dep_slot, fetch_list):
        levels, tracers, points, e_dev = tracer_old.shape
        cap = fetch_list.shape[2]
        assert levels == 1 and cap == LANES and tracers == SUB + 2 and points == 16
        rows = tracers * points
        vmem = pl.BlockSpec(memory_space=pltpu.VMEM)
        result = pl.pallas_call(
            functools.partial(kernel, sizes),
            out_shape=jax.ShapeDtypeStruct((rows, e_dev), jnp.float32),
            in_specs=[vmem] * 6,
            out_specs=vmem,
            scratch_shapes=[
                pltpu.VMEM((e_dev // LANES, rows, LANES), jnp.float32),
                pltpu.VMEM((e_dev // LANES, rows, LANES), jnp.float32),
                pltpu.VMEM((2, BAND // LANES, rows, LANES), jnp.float32),
                pltpu.VMEM((2, rows, LANES), jnp.float32),
                pltpu.VMEM((points, rows, e_dev), jnp.float32),
                pltpu.VMEM((e_dev // LANES, points * SUB, LANES), jnp.float32),
                pltpu.VMEM((4, e_dev // LANES, points, LANES), jnp.float32),
                pltpu.VMEM((e_dev // LANES, points, LANES), jnp.int32),
                pltpu.VMEM((e_dev // LANES, points, LANES), jnp.float32),
                pltpu.VMEM((2, 3, points, SUB, e_dev), jnp.float32),
                pltpu.VMEM((SUB, LANES), jnp.float32),
                pltpu.VMEM((n_all - 1, SUB, LANES), jnp.float32),
                pltpu.SemaphoreType.DMA((2, BAND // LANES)),
                pltpu.SemaphoreType.DMA((2, BAND // LANES)),
                pltpu.SemaphoreType.DMA,
                pltpu.SemaphoreType.DMA,
            ],
            compiler_params=pltpu.CompilerParams(collective_id=0, has_side_effects=True),
            name="transport",
        )(
            tracer_old.reshape(rows, e_dev),
            air_old.reshape(points, e_dev),
            air_new.reshape(points, e_dev),
            dep_coord.reshape(2, points, e_dev),
            dep_slot.reshape(points, e_dev),
            fetch_list.reshape(2, cap),
        )
        return result.reshape(levels, tracers, points, e_dev)

    return jax.shard_map(
        on_device,
        mesh=mesh,
        in_specs=(
            P("lev", None, None, "sfc"),
            P("lev", None, "sfc"),
            P("lev", None, "sfc"),
            P(None, "lev", None, "sfc"),
            P("lev", None, "sfc"),
            P("sfc", None, None),
        ),
        out_specs=P("lev", None, None, "sfc"),
        check_vma=False,
    )
```

```python
import functools

import jax
import jax.numpy as jnp
from jax import lax
from jax.experimental import pallas as pl
from jax.experimental.pallas import tpu as pltpu
from jax.sharding import PartitionSpec as P

BAND = 256
LANES = 128
SUB = 8
NODES = (-1.0, -0.4472135954999579, 0.4472135954999579, 1.0)
MESH = pl.DeviceIdType.MESH


def basis(coord):
    terms = []
    for first in range(4):
        term = None
        scale = 1.0
        for other in range(4):
            if other != first:
                factor = coord - NODES[other]
                term = factor if term is None else term * factor
                scale = scale / (NODES[first] - NODES[other])
        terms.append(term * scale)
    return terms


def lookup(values, index):
    return jnp.take_along_axis(values, index, axis=1, mode="promise_in_bounds")


def wide(row):
    return jnp.broadcast_to(row, (SUB, LANES))


def kernel(
    sizes, tr, air_old, air_new, coord, slot, fetch, out,
    natural, table, halo, side, part, along_a, along_b, places, masses, kept, message, heard,
    halo_send, halo_recv, sum_send, sum_recv, ready,
):
    n_sfc, n_lev = sizes
    n_all = n_sfc * n_lev
    points = slot.shape[0]
    e_dev = tr.shape[1]
    tracers = tr.shape[0] // points
    groups = e_dev // LANES
    row_groups = tr.shape[0] // SUB
    mains = points
    rests = row_groups - mains
    band_groups = BAND // LANES
    me_s, me_l = lax.axis_index("sfc"), lax.axis_index("lev")
    me = me_s * n_lev + me_l

    def spot(distance):
        other = lax.rem(me + distance, n_all)
        return (lax.div(other, n_lev), lax.rem(other, n_lev))

    barrier = pltpu.get_barrier_semaphore()

    def greet_s(distance, carry):
        pl.semaphore_signal(
            barrier, inc=1, device_id=(lax.rem(me_s + distance, n_sfc), me_l), device_id_type=MESH
        )
        return carry

    def greet_l(sem, distance, carry):
        pl.semaphore_signal(
            sem, inc=1, device_id=(me_s, lax.rem(me_l + distance, n_lev)), device_id_type=MESH
        )
        return carry

    lax.fori_loop(1, n_sfc, greet_s, 0)
    lax.fori_loop(1, n_lev, functools.partial(greet_l, barrier), 0)

    def cols(group):
        return pl.ds(group * LANES, LANES)

    def picked_rows(group):
        if group < mains:
            return pl.ds(group, SUB, stride=points)
        return pl.ds(SUB * points + group - mains, SUB, stride=rests)

    for g in range(groups):
        natural[g] = tr[:, cols(g)]
    for r in range(row_groups):
        for g in range(groups):
            table[g, pl.ds(r * SUB, SUB), :] = natural[g, picked_rows(r), :]
    for i, term in enumerate(basis(coord[0])):
        for g in range(groups):
            term_g = term[:, g * LANES : (g + 1) * LANES]
            along_a[g, pl.ds(i, points, stride=SUB), :] = term_g
            along_a[g, pl.ds(i + 4, points, stride=SUB), :] = term_g
    for i, term in enumerate(basis(coord[1])):
        for g in range(groups):
            along_b[i, g] = term[:, g * LANES : (g + 1) * LANES]
    for g in range(groups):
        places[g] = slot[:, cols(g)]
        masses[g] = air_new[:, cols(g)]

    def own(n, carry):
        rows = [wide(places[g, pl.ds(n, 1), :]) for g in range(groups)]
        lows = [row & (LANES - 1) for row in rows]
        highs = [row >> 7 for row in rows]
        for e in range(groups):
            for r in range(row_groups):
                here = pl.ds(r * SUB, SUB)
                value = lookup(table[0, here, :], lows[e])
                for g in range(1, groups):
                    value = jnp.where(highs[e] == g, lookup(table[g, here, :], lows[e]), value)
                part[n, here, cols(e)] = value
        return carry

    lax.fori_loop(0, points, own, 0, unroll=4)
    pl.semaphore_wait(barrier, n_sfc + n_lev - 2)
    lax.fori_loop(1, n_lev, functools.partial(greet_l, ready), 0)
    right = (lax.rem(me_s + 1, n_sfc), me_l)
    left = (lax.rem(me_s + n_sfc - 1, n_sfc), me_l)
    sends = []
    for k, (target, start) in enumerate(((right, e_dev - BAND), (left, 0))):
        for g in range(band_groups):
            send = pltpu.make_async_remote_copy(
                src_ref=tr.at[:, pl.ds(start + g * LANES, LANES)],
                dst_ref=halo.at[k, g],
                send_sem=halo_send.at[k, g],
                recv_sem=halo_recv.at[k, g],
                device_id=target,
                device_id_type=MESH,
            )
            send.start()
            sends.append(send)

    old_main = jnp.zeros((SUB, LANES), jnp.float32)
    for j in range(mains):
        for g in range(groups):
            old_main += table[g, pl.ds(j * SUB, SUB), :] * wide(air_old[pl.ds(j, 1), cols(g)])
    old_rest = []
    for t in range(SUB, tracers):
        product = tr[pl.ds(t * points, points), :] * air_old[...]
        old_rest.append(jnp.sum(jnp.sum(product, axis=1, keepdims=True), axis=0, keepdims=True))

    for k in range(2):
        for g in range(band_groups):
            sends[k * band_groups + g].wait()
        index = wide(fetch[pl.ds(k, 1), :])
        if k == 0:
            index = index - (e_dev - BAND)
        index_low, index_high = index & (LANES - 1), index >> 7
        for r in range(row_groups):
            value = lookup(halo[k, 0, picked_rows(r), :], index_low)
            for g in range(1, band_groups):
                value = jnp.where(
                    index_high == g, lookup(halo[k, g, picked_rows(r), :], index_low), value
                )
            side[k, pl.ds(r * SUB, SUB), :] = value

    def finish(n, carry):
        sums = list(carry)
        for e in range(groups):
            row = wide(places[e, pl.ds(n, 1), :])
            low_index, high_index = row & (LANES - 1), row >> 7
            in_left, in_right = high_index == groups, high_index == groups + 1
            mass = wide(masses[e, pl.ds(n, 1), :])

            def point(r):
                here = pl.ds(r * SUB, SUB)
                value = part[n, here, cols(e)]
                value = jnp.where(in_left, lookup(side[0, here, :], low_index), value)
                return jnp.where(in_right, lookup(side[1, here, :], low_index), value)

            terms_b = [wide(along_b[m, e, pl.ds(n, 1), :]) for m in range(4)]
            interp = low = high = None
            for i in range(4):
                inner = None
                for m in range(4):
                    value = point(4 * i + m)
                    low = value if low is None else jnp.minimum(low, value)
                    high = value if high is None else jnp.maximum(high, value)
                    scaled = terms_b[m] * value
                    inner = scaled if inner is None else inner + scaled
                term_a = wide(along_a[e, pl.ds(n * SUB + i, 1), :])
                inner = inner * term_a
                interp = inner if interp is None else interp + inner
            rest = low_rest = high_rest = None
            for q in range(rests):
                value = point(mains + q)
                low_rest = value if low_rest is None else jnp.minimum(low_rest, value)
                high_rest = value if high_rest is None else jnp.maximum(high_rest, value)
                scaled = terms_b[q] * value
                rest = scaled if rest is None else rest + scaled
            rest = rest * along_a[e, pl.ds(n * SUB, SUB), :]
            for shift in (1, 2):
                rest = rest + pltpu.roll(rest, SUB - shift, 0)
                low_rest = jnp.minimum(low_rest, pltpu.roll(low_rest, SUB - shift, 0))
                high_rest = jnp.maximum(high_rest, pltpu.roll(high_rest, SUB - shift, 0))
            for b, (value, least, most) in enumerate(
                ((interp, low, high), (rest, low_rest, high_rest))
            ):
                clipped = jnp.minimum(jnp.maximum(value, least), most)
                up, down = most - clipped, clipped - least
                for q, kind in enumerate((clipped, up, down)):
                    kept[b, q, n, :, cols(e)] = kind
                    sums[3 * b + q] = sums[3 * b + q] + mass * kind
        return tuple(sums)

    zero = jnp.zeros((SUB, LANES), jnp.float32)
    sums = lax.fori_loop(0, points, finish, (zero,) * 6, unroll=4)

    lane = lax.broadcasted_iota(jnp.int32, (SUB, LANES), 1)
    row = lax.broadcasted_iota(jnp.int32, (SUB, LANES), 0)
    packed = jnp.where(lane == 0, jnp.sum(old_main, axis=1, keepdims=True), 0.0)
    for b in range(2):
        for q in range(3):
            total = jnp.sum(sums[3 * b + q], axis=1, keepdims=True)
            packed = jnp.where(lane == 4 * b + q + 1, total, packed)
    for k, total in enumerate(old_rest):
        packed = jnp.where((lane == 4) & (row == 4 * k), total, packed)
    message[...] = packed

    def tell(distance, carry):
        pltpu.make_async_remote_copy(
            src_ref=message,
            dst_ref=heard.at[distance - 1],
            send_sem=sum_send,
            recv_sem=sum_recv,
            device_id=spot(distance),
            device_id_type=MESH,
        ).start()
        return carry

    pl.semaphore_wait(ready, n_lev - 1)
    lax.fori_loop(1, n_all, tell, 0)
    pltpu.make_async_copy(heard, heard, sum_recv).wait()
    total = packed
    for k in range(n_all - 1) if n_all <= 64 else ():
        total = total + heard[k]
    if n_all > 64:
        total = lax.fori_loop(0, n_all - 1, lambda k, acc: acc + heard[k], total)

    ups, gains = [], []
    for b in range(2):
        old, clip, up, down = [total[:, 4 * b + q : 4 * b + q + 1] for q in range(4)]
        shortfall = jnp.broadcast_to(old - clip, (SUB, LANES))
        is_up = shortfall >= 0
        room = jnp.where(is_up, jnp.broadcast_to(up, (SUB, LANES)), jnp.broadcast_to(down, (SUB, LANES)))
        ups.append(is_up)
        gains.append(shortfall / room)

    def fix(n, carry):
        for e in range(groups):
            done = []
            for b in range(2):
                clipped, up, down = [kept[b, q, n, :, cols(e)] for q in range(3)]
                done.append(clipped + gains[b] * jnp.where(ups[b], up, down))
            natural[e, pl.ds(n, SUB, stride=points), :] = done[0]
            for t in range(SUB, tracers):
                at = 4 * (t - SUB)
                natural[e, pl.ds(t * points + n, 1), :] = done[1][at : at + 1]
        return carry

    lax.fori_loop(0, points, fix, 0)
    for g in range(groups):
        out[:, cols(g)] = natural[g]
    pltpu.make_async_copy(heard, heard, sum_send).wait()


def solution(mesh):
    sizes = (mesh.shape["sfc"], mesh.shape["lev"])
    n_all = sizes[0] * sizes[1]

    def on_device(tracer_old, air_old, air_new, dep_coord, dep_slot, fetch_list):
        levels, tracers, points, e_dev = tracer_old.shape
        cap = fetch_list.shape[2]
        assert levels == 1 and cap == LANES and tracers == SUB + 2 and points == 16
        rows = tracers * points
        vmem = pl.BlockSpec(memory_space=pltpu.VMEM)
        result = pl.pallas_call(
            functools.partial(kernel, sizes),
            out_shape=pltpu.VMEM((rows, e_dev), jnp.float32),
            in_specs=[vmem] * 6,
            out_specs=vmem,
            scratch_shapes=[
                pltpu.VMEM((e_dev // LANES, rows, LANES), jnp.float32),
                pltpu.VMEM((e_dev // LANES, rows, LANES), jnp.float32),
                pltpu.VMEM((2, BAND // LANES, rows, LANES), jnp.float32),
                pltpu.VMEM((2, rows, LANES), jnp.float32),
                pltpu.VMEM((points, rows, e_dev), jnp.float32),
                pltpu.VMEM((e_dev // LANES, points * SUB, LANES), jnp.float32),
                pltpu.VMEM((4, e_dev // LANES, points, LANES), jnp.float32),
                pltpu.VMEM((e_dev // LANES, points, LANES), jnp.int32),
                pltpu.VMEM((e_dev // LANES, points, LANES), jnp.float32),
                pltpu.VMEM((2, 3, points, SUB, e_dev), jnp.float32),
                pltpu.VMEM((SUB, LANES), jnp.float32),
                pltpu.VMEM((n_all - 1, SUB, LANES), jnp.float32),
                pltpu.SemaphoreType.DMA((2, BAND // LANES)),
                pltpu.SemaphoreType.DMA((2, BAND // LANES)),
                pltpu.SemaphoreType.DMA,
                pltpu.SemaphoreType.DMA,
                pltpu.SemaphoreType.REGULAR,
            ],
            compiler_params=pltpu.CompilerParams(collective_id=0, has_side_effects=True),
            name="transport",
        )(
            tracer_old.reshape(rows, e_dev),
            air_old.reshape(points, e_dev),
            air_new.reshape(points, e_dev),
            dep_coord.reshape(2, points, e_dev),
            dep_slot.reshape(points, e_dev),
            fetch_list.reshape(2, cap),
        )
        return result.reshape(levels, tracers, points, e_dev)

    return jax.shard_map(
        on_device,
        mesh=mesh,
        in_specs=(
            P("lev", None, None, "sfc"),
            P("lev", None, "sfc"),
            P("lev", None, "sfc"),
            P(None, "lev", None, "sfc"),
            P("lev", None, "sfc"),
            P("sfc", None, None),
        ),
        out_specs=P("lev", None, None, "sfc"),
        check_vma=False,
    )
```

```python
import functools

import jax
import jax.numpy as jnp
from jax import lax
from jax.experimental import pallas as pl
from jax.experimental.pallas import tpu as pltpu
from jax.sharding import PartitionSpec as P

BAND = 256
LANES = 128
SUB = 8
NODES = (-1.0, -0.4472135954999579, 0.4472135954999579, 1.0)
MESH = pl.DeviceIdType.MESH


def basis(coord):
    terms = []
    for first in range(4):
        term = None
        scale = 1.0
        for other in range(4):
            if other != first:
                factor = coord - NODES[other]
                term = factor if term is None else term * factor
                scale = scale / (NODES[first] - NODES[other])
        terms.append(term * scale)
    return terms


def lookup(values, index):
    return jnp.take_along_axis(values, index, axis=1, mode="promise_in_bounds")


def wide(row):
    return jnp.broadcast_to(row, (SUB, LANES))


def kernel(
    sizes, tr, air_old, air_new, coord, slot, fetch, out,
    natural, table, halo, side, along_a, along_b, places, masses, masses_old, coords, wanted,
    kept, message, heard, load_sem, halo_send, halo_recv, sum_send, sum_recv, ready,
):
    n_sfc, n_lev = sizes
    n_all = n_sfc * n_lev
    points = slot.shape[0]
    e_dev = tr.shape[1]
    tracers = tr.shape[0] // points
    groups = e_dev // LANES
    row_groups = tr.shape[0] // SUB
    mains = points
    rests = row_groups - mains
    band_groups = BAND // LANES
    me_s, me_l = lax.axis_index("sfc"), lax.axis_index("lev")
    me = me_s * n_lev + me_l

    def spot(distance):
        other = lax.rem(me + distance, n_all)
        return (lax.div(other, n_lev), lax.rem(other, n_lev))

    barrier = pltpu.get_barrier_semaphore()

    def greet_s(distance, carry):
        pl.semaphore_signal(
            barrier, inc=1, device_id=(lax.rem(me_s + distance, n_sfc), me_l), device_id_type=MESH
        )
        return carry

    def greet_l(sem, distance, carry):
        pl.semaphore_signal(
            sem, inc=1, device_id=(me_s, lax.rem(me_l + distance, n_lev)), device_id_type=MESH
        )
        return carry

    lax.fori_loop(1, n_sfc, greet_s, 0)
    lax.fori_loop(1, n_lev, functools.partial(greet_l, barrier), 0)

    def cols(group):
        return pl.ds(group * LANES, LANES)

    loads = []

    def load(source, target):
        copy = pltpu.make_async_copy(source, target, load_sem.at[len(loads)])
        copy.start()
        loads.append(copy)

    for g in range(groups):
        load(tr.at[:, cols(g)], natural.at[g])
        load(slot.at[:, cols(g)], places.at[g])
        load(coord.at[:, :, cols(g)], coords.at[g])
    for g in range(groups):
        load(air_old.at[:, cols(g)], masses_old.at[g])
        load(air_new.at[:, cols(g)], masses.at[g])
    load(fetch, wanted)

    def picked_rows(group):
        if group < mains:
            return pl.ds(group, SUB, stride=points)
        return pl.ds(SUB * points + group - mains, SUB, stride=rests)

    def prepare():
        for copy in loads:
            copy.wait()
        for r in range(row_groups):
            for g in range(groups):
                table[g, pl.ds(r * SUB, SUB), :] = natural[g, picked_rows(r), :]
        for g in range(groups):
            for i, term in enumerate(basis(coords[g, 0])):
                along_a[g, pl.ds(i, points, stride=SUB), :] = term
                along_a[g, pl.ds(i + 4, points, stride=SUB), :] = term
            for i, term in enumerate(basis(coords[g, 1])):
                along_b[i, g] = term

    def shares(point, n, e):
        terms_b = [wide(along_b[m, e, pl.ds(n, 1), :]) for m in range(4)]
        interp = low = high = None
        for i in range(4):
            inner = None
            for m in range(4):
                value = point(4 * i + m)
                low = value if low is None else jnp.minimum(low, value)
                high = value if high is None else jnp.maximum(high, value)
                scaled = terms_b[m] * value
                inner = scaled if inner is None else inner + scaled
            inner = inner * wide(along_a[e, pl.ds(n * SUB + i, 1), :])
            interp = inner if interp is None else interp + inner
        rest = low_rest = high_rest = None
        for q in range(rests):
            value = point(mains + q)
            low_rest = value if low_rest is None else jnp.minimum(low_rest, value)
            high_rest = value if high_rest is None else jnp.maximum(high_rest, value)
            scaled = terms_b[q] * value
            rest = scaled if rest is None else rest + scaled
        rest = rest * along_a[e, pl.ds(n * SUB, SUB), :]
        return (interp, low, high), (rest, low_rest, high_rest)

    def own(n, carry):
        for e in range(groups):
            row = wide(places[e, pl.ds(n, 1), :])
            low_index, high_index = row & (LANES - 1), row >> 7
            above = [high_index == g for g in range(1, groups)]

            def point(r):
                here = pl.ds(r * SUB, SUB)
                value = lookup(table[0, here, :], low_index)
                for g in range(1, groups):
                    value = jnp.where(above[g - 1], lookup(table[g, here, :], low_index), value)
                return value

            for b, kinds in enumerate(shares(point, n, e)):
                for q, kind in enumerate(kinds):
                    kept[b, q, n, :, cols(e)] = kind
        return carry

    def receive(k):
        for g in range(band_groups):
            pltpu.make_async_copy(halo.at[k, g], halo.at[k, g], halo_recv.at[k, g]).wait()
        index = wide(wanted[pl.ds(k, 1), :]) - jnp.where(k == 0, e_dev - BAND, 0)
        index_low, index_high = index & (LANES - 1), index >> 7
        for r in range(row_groups):
            value = lookup(halo[k, 0, picked_rows(r), :], index_low)
            for g in range(1, band_groups):
                value = jnp.where(
                    index_high == g, lookup(halo[k, g, picked_rows(r), :], index_low), value
                )
            side[pl.ds(r * SUB, SUB), :] = value

    def merged(k, n, e):
        row = wide(places[e, pl.ds(n, 1), :])
        low_index, mine = row & (LANES - 1), (row >> 7) == groups + k

        def point(r):
            return lookup(side[pl.ds(r * SUB, SUB), :], low_index)

        return [
            [jnp.where(mine, kind, kept[b, q, n, :, cols(e)]) for q, kind in enumerate(kinds)]
            for b, kinds in enumerate(shares(point, n, e))
        ]

    def near_pass(k, n, carry):
        for e in range(groups):
            for b, kinds in enumerate(merged(k, n, e)):
                for q, kind in enumerate(kinds):
                    kept[b, q, n, :, cols(e)] = kind
        return carry

    def far_pass(k, n, carry):
        sums = list(carry)
        for e in range(groups):
            mass = wide(masses[e, pl.ds(n, 1), :])
            for b, (value, least, most) in enumerate(merged(k, n, e)):
                for shift in (1, 2) if b else ():
                    value = value + pltpu.roll(value, SUB - shift, 0)
                    least = jnp.minimum(least, pltpu.roll(least, SUB - shift, 0))
                    most = jnp.maximum(most, pltpu.roll(most, SUB - shift, 0))
                clipped = jnp.minimum(jnp.maximum(value, least), most)
                for q, kind in enumerate((clipped, most - clipped, clipped - least)):
                    kept[b, q, n, :, cols(e)] = kind
                    sums[3 * b + q] = sums[3 * b + q] + mass * kind
        return tuple(sums)

    early = points // 4
    prepare()
    lax.fori_loop(0, early, own, 0, unroll=4)
    pl.semaphore_wait(barrier, n_sfc + n_lev - 2)
    right = (lax.rem(me_s + 1, n_sfc), me_l)
    left = (lax.rem(me_s + n_sfc - 1, n_sfc), me_l)
    sends = []
    for k, (target, start) in enumerate(((right, e_dev - BAND), (left, 0))):
        for g in range(band_groups):
            send = pltpu.make_async_remote_copy(
                src_ref=tr.at[:, pl.ds(start + g * LANES, LANES)],
                dst_ref=halo.at[k, g],
                send_sem=halo_send.at[k, g],
                recv_sem=halo_recv.at[k, g],
                device_id=target,
                device_id_type=MESH,
            )
            send.start()
            sends.append(send)
    lax.fori_loop(1, n_lev, functools.partial(greet_l, ready), 0)
    lax.fori_loop(early, points, own, 0, unroll=4)

    lane = lax.broadcasted_iota(jnp.int32, (SUB, LANES), 1)
    row = lax.broadcasted_iota(jnp.int32, (SUB, LANES), 0)
    old_main = jnp.zeros((SUB, LANES), jnp.float32)
    for j in range(mains):
        for g in range(groups):
            old_main += table[g, pl.ds(j * SUB, SUB), :] * wide(masses_old[g, pl.ds(j, 1), :])
    packed = jnp.where(lane == row, jnp.sum(old_main, axis=1, keepdims=True), 0.0)
    for t in range(SUB, tracers):
        product = sum(natural[g, pl.ds(t * points, points), :] * masses_old[g] for g in range(groups))
        total = jnp.sum(jnp.sum(product, axis=1, keepdims=True), axis=0, keepdims=True)
        at = 4 * (t - SUB)
        packed = jnp.where((lane == 4 * SUB + row) & (row == at), total, packed)

    far = lax.rem(me_s, 2)
    near = 1 - far
    receive(near)
    lax.fori_loop(0, points, functools.partial(near_pass, near), 0, unroll=4)
    receive(far)
    zero = jnp.zeros((SUB, LANES), jnp.float32)
    sums = lax.fori_loop(0, points, functools.partial(far_pass, far), (zero,) * 6, unroll=4)

    for b in range(2):
        for q in range(3):
            total = jnp.sum(sums[3 * b + q], axis=1, keepdims=True)
            packed = jnp.where(lane == (4 * b + q + 1) * SUB + row, total, packed)
    packed = jnp.sum(packed, axis=0, keepdims=True)
    message[...] = packed

    pl.semaphore_wait(ready, n_lev - 1)

    def tell(distance, carry):
        pltpu.make_async_remote_copy(
            src_ref=message,
            dst_ref=heard.at[distance - 1],
            send_sem=sum_send,
            recv_sem=sum_recv,
            device_id=spot(distance),
            device_id_type=MESH,
        ).start()
        return carry

    lax.fori_loop(1, n_all, tell, 0)
    pltpu.make_async_copy(heard, heard, sum_recv).wait()
    total = packed
    for k in range(n_all - 1) if n_all <= 64 else ():
        total = total + heard[k]
    if n_all > 64:
        total = lax.fori_loop(0, n_all - 1, lambda k, acc: acc + heard[k], total)

    old, clip, up, down = [
        wide(total) if q == 0 else pltpu.roll(wide(total), LANES - q * SUB, 1) for q in range(4)
    ]
    shortfall = old - clip
    raised = jnp.where(shortfall >= 0, shortfall / up, 0.0)
    lowered = jnp.where(shortfall >= 0, 0.0, shortfall / down)
    gains = []
    for b in range(2):
        pair = []
        for gain in (raised, lowered):
            column = jnp.where(lane == 4 * b * SUB + row, gain, 0.0)
            pair.append(jnp.broadcast_to(jnp.sum(column, axis=1, keepdims=True), (SUB, LANES)))
        gains.append(pair)

    def fix(n, carry):
        for e in range(groups):
            done = []
            for b in range(2):
                clipped, up, down = [kept[b, q, n, :, cols(e)] for q in range(3)]
                done.append(clipped + (gains[b][0] * up + gains[b][1] * down))
            natural[e, pl.ds(n, SUB, stride=points), :] = done[0]
            for t in range(SUB, tracers):
                at = 4 * (t - SUB)
                natural[e, pl.ds(t * points + n, 1), :] = done[1][at : at + 1]
        return carry

    lax.fori_loop(0, points, fix, 0, unroll=2)
    for g in range(groups):
        out[:, cols(g)] = natural[g]
    for send in sends:
        send.wait_send()
    pltpu.make_async_copy(heard, heard, sum_send).wait()


def solution(mesh):
    sizes = (mesh.shape["sfc"], mesh.shape["lev"])
    n_all = sizes[0] * sizes[1]

    def on_device(tracer_old, air_old, air_new, dep_coord, dep_slot, fetch_list):
        levels, tracers, points, e_dev = tracer_old.shape
        cap = fetch_list.shape[2]
        assert levels == 1 and cap == LANES and tracers == SUB + 2 and points == 16
        rows = tracers * points
        groups = e_dev // LANES
        vmem = pl.BlockSpec(memory_space=pltpu.VMEM)
        result = pl.pallas_call(
            functools.partial(kernel, sizes),
            out_shape=pltpu.VMEM((rows, e_dev), jnp.float32),
            in_specs=[pl.BlockSpec(memory_space=pl.ANY)] * 6,
            out_specs=vmem,
            scratch_shapes=[
                pltpu.VMEM((groups, rows, LANES), jnp.float32),
                pltpu.VMEM((groups, rows, LANES), jnp.float32),
                pltpu.VMEM((2, BAND // LANES, rows, LANES), jnp.float32),
                pltpu.VMEM((rows, LANES), jnp.float32),
                pltpu.VMEM((groups, points * SUB, LANES), jnp.float32),
                pltpu.VMEM((4, groups, points, LANES), jnp.float32),
                pltpu.VMEM((groups, points, LANES), jnp.int32),
                pltpu.VMEM((groups, points, LANES), jnp.float32),
                pltpu.VMEM((groups, points, LANES), jnp.float32),
                pltpu.VMEM((groups, 2, points, LANES), jnp.float32),
                pltpu.VMEM((2, cap), jnp.int32),
                pltpu.VMEM((2, 3, points, SUB, e_dev), jnp.float32),
                pltpu.VMEM((1, LANES), jnp.float32),
                pltpu.VMEM((n_all - 1, 1, LANES), jnp.float32),
                pltpu.SemaphoreType.DMA((5 * groups + 1,)),
                pltpu.SemaphoreType.DMA((2, BAND // LANES)),
                pltpu.SemaphoreType.DMA((2, BAND // LANES)),
                pltpu.SemaphoreType.DMA,
                pltpu.SemaphoreType.DMA,
                pltpu.SemaphoreType.REGULAR,
            ],
            compiler_params=pltpu.CompilerParams(collective_id=0, has_side_effects=True),
            name="transport",
        )(
            tracer_old.reshape(rows, e_dev),
            air_old.reshape(points, e_dev),
            air_new.reshape(points, e_dev),
            dep_coord.reshape(2, points, e_dev),
            dep_slot.reshape(points, e_dev),
            fetch_list.reshape(2, cap),
        )
        return result.reshape(levels, tracers, points, e_dev)

    return jax.shard_map(
        on_device,
        mesh=mesh,
        in_specs=(
            P("lev", None, None, "sfc"),
            P("lev", None, "sfc"),
            P("lev", None, "sfc"),
            P(None, "lev", None, "sfc"),
            P("lev", None, "sfc"),
            P("sfc", None, None),
        ),
        out_specs=P("lev", None, None, "sfc"),
        check_vma=False,
    )
```

```python
import functools

import jax
import jax.numpy as jnp
from jax import lax
from jax.experimental import pallas as pl
from jax.experimental.pallas import tpu as pltpu
from jax.sharding import PartitionSpec as P

BAND = 256
LANES = 128
SUB = 8
NODES = (-1.0, -0.4472135954999579, 0.4472135954999579, 1.0)
MESH = pl.DeviceIdType.MESH


def basis(coord):
    terms = []
    for first in range(4):
        term = None
        scale = 1.0
        for other in range(4):
            if other != first:
                factor = coord - NODES[other]
                term = factor if term is None else term * factor
                scale = scale / (NODES[first] - NODES[other])
        terms.append(term * scale)
    return terms


def lookup(values, index):
    return jnp.take_along_axis(values, index, axis=1, mode="promise_in_bounds")


def wide(row):
    return jnp.broadcast_to(row, (SUB, LANES))


def kernel(
    sizes, tr, air_old, air_new, coord, slot, fetch, out,
    natural, stage, table, halo, side, along_a, along_b, mixed_a, mixed_b, places, masses, masses_old, coords, wanted,
    kept, begun, message, heard, load_sem, halo_send, halo_recv, sum_send, sum_recv, ready,
):
    n_sfc, n_lev = sizes
    n_all = n_sfc * n_lev
    points = slot.shape[0]
    tracers, _, e_dev = tr.shape
    groups = e_dev // LANES
    row_groups = tracers * points // SUB
    halves = points // SUB
    flat = tracers * SUB
    mains = points
    rests = row_groups - mains
    band_groups = BAND // LANES
    me_s, me_l = lax.axis_index("sfc"), lax.axis_index("lev")
    me = me_s * n_lev + me_l

    def spot(distance):
        other = lax.rem(me + distance, n_all)
        return (lax.div(other, n_lev), lax.rem(other, n_lev))

    barrier = pltpu.get_barrier_semaphore()

    def greet_s(distance, carry):
        pl.semaphore_signal(
            barrier, inc=1, device_id=(lax.rem(me_s + distance, n_sfc), me_l), device_id_type=MESH
        )
        return carry

    def greet_l(sem, distance, carry):
        pl.semaphore_signal(
            sem, inc=1, device_id=(me_s, lax.rem(me_l + distance, n_lev)), device_id_type=MESH
        )
        return carry

    lax.fori_loop(1, n_sfc, greet_s, 0)
    lax.fori_loop(1, n_lev, functools.partial(greet_l, barrier), 0)

    def cols(group):
        return pl.ds(group * LANES, LANES)

    loads = []

    def load(source, target):
        copy = pltpu.make_async_copy(source, target, load_sem.at[len(loads)])
        copy.start()
        loads.append(copy)

    for g in range(groups):
        for h in range(halves):
            load(tr.at[:, pl.ds(h * SUB, SUB), cols(g)], natural.at[g, h])
        load(slot.at[:, cols(g)], places.at[g])
        load(coord.at[:, :, cols(g)], coords.at[g])
    for g in range(groups):
        load(air_old.at[:, cols(g)], masses_old.at[g])
        load(air_new.at[:, cols(g)], masses.at[g])
    load(fetch, wanted)

    def picked_rows(group):
        if group < mains:
            return pl.ds(group % SUB, SUB, stride=SUB)
        return pl.ds(SUB * SUB + (group - mains) % 2, SUB, stride=2)

    def half_of(h):
        return list(range(SUB * h, SUB * h + SUB)) + [mains + 2 * h, mains + 2 * h + 1]

    def prepare():
        for copy in loads:
            copy.wait()
        for h in range(halves):
            for g in range(groups):
                block = natural.at[g, h].reshape(flat, LANES)
                for r in half_of(h):
                    table[g, pl.ds(r * SUB, SUB), :] = block[picked_rows(r), :]
        for g in range(groups):
            for i, term in enumerate(basis(coords[g, 0])):
                along_a[i, g] = term
                for s in (0, 1, 4, 5):
                    mixed_a[i // 2, g, pl.ds(s + 2 * (i % 2), points, stride=SUB), :] = term
            for m, term in enumerate(basis(coords[g, 1])):
                along_b[m, g] = term
                for s in (0, 2, 4, 6):
                    mixed_b[m % 2, g, pl.ds(s + m // 2, points, stride=SUB), :] = term

    def half_shares(point, n, e, h):
        terms_b = [wide(along_b[m, e, pl.ds(n, 1), :]) for m in range(4)]
        interp = low = high = None
        for i in (2 * h, 2 * h + 1):
            inner = None
            for m in range(4):
                value = point(4 * i + m)
                low = value if low is None else jnp.minimum(low, value)
                high = value if high is None else jnp.maximum(high, value)
                scaled = terms_b[m] * value
                inner = scaled if inner is None else inner + scaled
            inner = inner * wide(along_a[i, e, pl.ds(n, 1), :])
            interp = inner if interp is None else interp + inner
        rest = low_rest = high_rest = None
        for q in range(2):
            value = point(mains + 2 * h + q)
            low_rest = value if low_rest is None else jnp.minimum(low_rest, value)
            high_rest = value if high_rest is None else jnp.maximum(high_rest, value)
            scaled = mixed_b[q, e, pl.ds(n * SUB, SUB), :] * value
            rest = scaled if rest is None else rest + scaled
        rest = rest * mixed_a[h, e, pl.ds(n * SUB, SUB), :]
        return (interp, low, high), (rest, low_rest, high_rest)

    def joined(one, two):
        return [
            (a[0] + b[0], jnp.minimum(a[1], b[1]), jnp.maximum(a[2], b[2])) for a, b in zip(one, two)
        ]

    def shares(point, n, e):
        return joined(half_shares(point, n, e, 0), half_shares(point, n, e, 1))

    def own(n, carry):
        for e in range(groups):
            row = wide(places[e, pl.ds(n, 1), :])
            low_index, high_index = row & (LANES - 1), row >> 7
            above = [high_index == g for g in range(1, groups)]

            def point(r):
                here = pl.ds(r * SUB, SUB)
                value = lookup(table[0, here, :], low_index)
                for g in range(1, groups):
                    value = jnp.where(above[g - 1], lookup(table[g, here, :], low_index), value)
                return value

            for b, kinds in enumerate(shares(point, n, e)):
                for q, kind in enumerate(kinds):
                    kept[b, q, n, :, cols(e)] = kind
        return carry

    def receive(k, h):
        for g in range(band_groups):
            pltpu.make_async_copy(halo.at[k, g, h], halo.at[k, g, h], halo_recv.at[k, g, h]).wait()
        index = wide(wanted[pl.ds(k, 1), :]) - jnp.where(k == 0, e_dev - BAND, 0)
        index_low, index_high = index & (LANES - 1), index >> 7
        blocks = [halo.at[k, g, h].reshape(flat, LANES) for g in range(band_groups)]
        for r in half_of(h):
            value = lookup(blocks[0][picked_rows(r), :], index_low)
            for g in range(1, band_groups):
                value = jnp.where(
                    index_high == g, lookup(blocks[g][picked_rows(r), :], index_low), value
                )
            side[pl.ds(r * SUB, SUB), :] = value

    def chosen(k, n, e):
        row = wide(places[e, pl.ds(n, 1), :])
        low_index, mine = row & (LANES - 1), (row >> 7) == groups + k

        def point(r):
            return lookup(side[pl.ds(r * SUB, SUB), :], low_index)

        def merge(found):
            return [
                [jnp.where(mine, kind, kept[b, q, n, :, cols(e)]) for q, kind in enumerate(kinds)]
                for b, kinds in enumerate(found)
            ]

        return point, merge

    def near_pass(k, n, carry):
        for e in range(groups):
            point, merge = chosen(k, n, e)
            for b, kinds in enumerate(merge(shares(point, n, e))):
                for q, kind in enumerate(kinds):
                    kept[b, q, n, :, cols(e)] = kind
        return carry

    def begin_pass(k, n, carry):
        for e in range(groups):
            point, _ = chosen(k, n, e)
            for b, kinds in enumerate(half_shares(point, n, e, 0)):
                for q, kind in enumerate(kinds):
                    begun[b, q, n, :, cols(e)] = kind
        return carry

    def far_pass(k, n, carry):
        sums = list(carry)
        for e in range(groups):
            mass = wide(masses[e, pl.ds(n, 1), :])
            point, merge = chosen(k, n, e)
            first = [[begun[b, q, n, :, cols(e)] for q in range(3)] for b in range(2)]
            found = joined(first, half_shares(point, n, e, 1))
            for b, (value, least, most) in enumerate(merge(found)):
                for shift in (1, 2) if b else ():
                    value = value + pltpu.roll(value, SUB - shift, 0)
                    least = jnp.minimum(least, pltpu.roll(least, SUB - shift, 0))
                    most = jnp.maximum(most, pltpu.roll(most, SUB - shift, 0))
                clipped = jnp.minimum(jnp.maximum(value, least), most)
                for q, kind in enumerate((clipped, most - clipped, clipped - least)):
                    kept[b, q, n, :, cols(e)] = kind
                    sums[3 * b + q] = sums[3 * b + q] + mass * kind
        return tuple(sums)

    early = points // 2
    prepare()
    lax.fori_loop(0, early, own, 0, unroll=4)
    pl.semaphore_wait(barrier, n_sfc + n_lev - 2)
    right = (lax.rem(me_s + 1, n_sfc), me_l)
    left = (lax.rem(me_s + n_sfc - 1, n_sfc), me_l)
    sends = []
    for h in range(halves):
        for k, (target, start) in enumerate(((right, e_dev - BAND), (left, 0))):
            for g in range(band_groups):
                send = pltpu.make_async_remote_copy(
                    src_ref=tr.at[:, pl.ds(h * SUB, SUB), pl.ds(start + g * LANES, LANES)],
                    dst_ref=halo.at[k, g, h],
                    send_sem=halo_send.at[k, g, h],
                    recv_sem=halo_recv.at[k, g, h],
                    device_id=target,
                    device_id_type=MESH,
                )
                send.start()
                sends.append(send)
    lax.fori_loop(1, n_lev, functools.partial(greet_l, ready), 0)
    lax.fori_loop(early, points, own, 0, unroll=4)

    lane = lax.broadcasted_iota(jnp.int32, (SUB, LANES), 1)
    row = lax.broadcasted_iota(jnp.int32, (SUB, LANES), 0)
    old_main = jnp.zeros((SUB, LANES), jnp.float32)
    for j in range(mains):
        for g in range(groups):
            old_main += table[g, pl.ds(j * SUB, SUB), :] * wide(masses_old[g, pl.ds(j, 1), :])
    packed = jnp.where(lane == row, jnp.sum(old_main, axis=1, keepdims=True), 0.0)
    for t in range(SUB, tracers):
        product = sum(
            natural[g, h, t] * masses_old[g, pl.ds(h * SUB, SUB), :]
            for g in range(groups)
            for h in range(halves)
        )
        total = jnp.sum(jnp.sum(product, axis=1, keepdims=True), axis=0, keepdims=True)
        at = 4 * (t - SUB)
        packed = jnp.where((lane == 4 * SUB + row) & (row == at), total, packed)

    far = lax.rem(me_s, 2)
    near = 1 - far
    for h in range(halves):
        receive(near, h)
    lax.fori_loop(0, points, functools.partial(near_pass, near), 0, unroll=4)
    receive(far, 0)
    lax.fori_loop(0, points, functools.partial(begin_pass, far), 0, unroll=4)
    receive(far, 1)
    zero = jnp.zeros((SUB, LANES), jnp.float32)
    sums = lax.fori_loop(0, points, functools.partial(far_pass, far), (zero,) * 6, unroll=4)

    for b in range(2):
        for q in range(3):
            total = jnp.sum(sums[3 * b + q], axis=1, keepdims=True)
            packed = jnp.where(lane == (4 * b + q + 1) * SUB + row, total, packed)
    packed = jnp.sum(packed, axis=0, keepdims=True)
    message[...] = packed

    pl.semaphore_wait(ready, n_lev - 1)

    def tell(distance, carry):
        pltpu.make_async_remote_copy(
            src_ref=message,
            dst_ref=heard.at[distance - 1],
            send_sem=sum_send,
            recv_sem=sum_recv,
            device_id=spot(distance),
            device_id_type=MESH,
        ).start()
        return carry

    lax.fori_loop(1, n_all, tell, 0)
    pltpu.make_async_copy(heard, heard, sum_recv).wait()
    total = packed
    for k in range(n_all - 1) if n_all <= 64 else ():
        total = total + heard[k]
    if n_all > 64:
        total = lax.fori_loop(0, n_all - 1, lambda k, acc: acc + heard[k], total)

    old, clip, up, down = [
        wide(total) if q == 0 else pltpu.roll(wide(total), LANES - q * SUB, 1) for q in range(4)
    ]
    shortfall = old - clip
    raised = jnp.where(shortfall >= 0, shortfall / up, 0.0)
    lowered = jnp.where(shortfall >= 0, 0.0, shortfall / down)
    gains = []
    for b in range(2):
        pair = []
        for gain in (raised, lowered):
            column = jnp.where(lane == 4 * b * SUB + row, gain, 0.0)
            pair.append(jnp.broadcast_to(jnp.sum(column, axis=1, keepdims=True), (SUB, LANES)))
        gains.append(pair)

    def fix(n, carry):
        for e in range(groups):
            done = []
            for b in range(2):
                clipped, up, down = [kept[b, q, n, :, cols(e)] for q in range(3)]
                done.append(clipped + (gains[b][0] * up + gains[b][1] * down))
            stage[e, pl.ds(n, SUB, stride=points), :] = done[0]
            for t in range(SUB, tracers):
                at = 4 * (t - SUB)
                stage[e, pl.ds(t * points + n, 1), :] = done[1][at : at + 1]
        return carry

    lax.fori_loop(0, points, fix, 0, unroll=2)
    for g in range(groups):
        out[:, cols(g)] = stage[g]
    for send in sends:
        send.wait_send()
    pltpu.make_async_copy(heard, heard, sum_send).wait()


def solution(mesh):
    sizes = (mesh.shape["sfc"], mesh.shape["lev"])
    n_all = sizes[0] * sizes[1]

    def on_device(tracer_old, air_old, air_new, dep_coord, dep_slot, fetch_list):
        levels, tracers, points, e_dev = tracer_old.shape
        cap = fetch_list.shape[2]
        assert levels == 1 and cap == LANES and tracers == SUB + 2 and points == 16
        rows = tracers * points
        groups, halves = e_dev // LANES, points // SUB
        vmem = pl.BlockSpec(memory_space=pltpu.VMEM)
        result = pl.pallas_call(
            functools.partial(kernel, sizes),
            out_shape=pltpu.VMEM((rows, e_dev), jnp.float32),
            in_specs=[pl.BlockSpec(memory_space=pl.ANY)] * 6,
            out_specs=vmem,
            scratch_shapes=[
                pltpu.VMEM((groups, halves, tracers, SUB, LANES), jnp.float32),
                pltpu.VMEM((groups, rows, LANES), jnp.float32),
                pltpu.VMEM((groups, rows, LANES), jnp.float32),
                pltpu.VMEM((2, BAND // LANES, halves, tracers, SUB, LANES), jnp.float32),
                pltpu.VMEM((rows, LANES), jnp.float32),
                pltpu.VMEM((4, groups, points, LANES), jnp.float32),
                pltpu.VMEM((4, groups, points, LANES), jnp.float32),
                pltpu.VMEM((2, groups, points * SUB, LANES), jnp.float32),
                pltpu.VMEM((2, groups, points * SUB, LANES), jnp.float32),
                pltpu.VMEM((groups, points, LANES), jnp.int32),
                pltpu.VMEM((groups, points, LANES), jnp.float32),
                pltpu.VMEM((groups, points, LANES), jnp.float32),
                pltpu.VMEM((groups, 2, points, LANES), jnp.float32),
                pltpu.VMEM((2, cap), jnp.int32),
                pltpu.VMEM((2, 3, points, SUB, e_dev), jnp.float32),
                pltpu.VMEM((2, 3, points, SUB, e_dev), jnp.float32),
                pltpu.VMEM((1, LANES), jnp.float32),
                pltpu.VMEM((n_all - 1, 1, LANES), jnp.float32),
                pltpu.SemaphoreType.DMA(((4 + halves) * groups + 1,)),
                pltpu.SemaphoreType.DMA((2, BAND // LANES, halves)),
                pltpu.SemaphoreType.DMA((2, BAND // LANES, halves)),
                pltpu.SemaphoreType.DMA,
                pltpu.SemaphoreType.DMA,
                pltpu.SemaphoreType.REGULAR,
            ],
            compiler_params=pltpu.CompilerParams(collective_id=0, has_side_effects=True),
            name="transport",
        )(
            tracer_old.reshape(tracers, points, e_dev),
            air_old.reshape(points, e_dev),
            air_new.reshape(points, e_dev),
            dep_coord.reshape(2, points, e_dev),
            dep_slot.reshape(points, e_dev),
            fetch_list.reshape(2, cap),
        )
        return result.reshape(levels, tracers, points, e_dev)

    return jax.shard_map(
        on_device,
        mesh=mesh,
        in_specs=(
            P("lev", None, None, "sfc"),
            P("lev", None, "sfc"),
            P("lev", None, "sfc"),
            P(None, "lev", None, "sfc"),
            P("lev", None, "sfc"),
            P("sfc", None, None),
        ),
        out_specs=P("lev", None, None, "sfc"),
        check_vma=False,
    )
```
